32 devices in a mesh: dp: 8 (over z, x), section: 4 (over y, core).
Axes of the slice: x: 2, y: 2, z: 4, core: 2. Of those that a mesh axis runs over, the one named last changes fastest.
Arguments:
- activations: bfloat16 [4, 16, 512, 4096], P('section', 'dp'), may hold values from -16 to 16
- out_grads: bfloat16 [4, 16, 512, 1024], P('section', 'dp'), may hold values from -16 to 16
- lengths: int32 [16], P('dp'), may hold values from 64 to 512, as said below
Outputs:
- mean_grad: bfloat16 [4, 4096, 1024], P('section', 'dp')
- norm_ratio: float32 [16], P('dp')
The draws below stay inside these ranges and needn't reach their ends.
Inputs may be any that keep to these rules, and one draw needn't show every extreme that they name: Example e's first lengths[e] token slots are real, the rest padding; some example fills all 512 slots.
All inputs are finite; a program needn't handle non-finite values.
Results may differ from the reference program's by a relative error of at most 0.015.
Values may be sent and summed in bfloat16 or wider, within the bound.
A program may use at most 128 MiB of HBM per device.

```python
import math
import jax
import jax.numpy as jnp
from jax import lax

D = 4096
KV = 1024
SEQ = 512
EX_DEV = 2
LAYERS = 4
EXAMPLES = 16
N_DP = 8


def feature_values(key, shape):
    base_key, scale_key, common_key, row_key = jax.random.split(key, 4)
    values = jax.random.normal(base_key, shape, jnp.float32)
    layer_scale = jax.random.uniform(scale_key, (shape[0], shape[1], 1, 1), jnp.float32, 0.5, 2.0)
    return values * layer_scale


def example_order(key):
    length_key, ranking_key = jax.random.split(jax.random.fold_in(key, 37))
    ranking = jax.random.permutation(ranking_key, EXAMPLES)
    return (length_key, ranking)


def draw_activations(key, part):
    values = feature_values(jax.random.fold_in(key, 11), (LAYERS, EXAMPLES, SEQ, D))
    return jnp.clip(values, -16.0, 16.0).astype(jnp.bfloat16)


def draw_out_grads(key, part):
    values = feature_values(jax.random.fold_in(key, 23), (LAYERS, EXAMPLES, SEQ, KV))
    length_key, ranking = example_order(key)
    log_factor = jax.random.uniform(jax.random.fold_in(key, 41), (EXAMPLES,), jnp.float32, jnp.log(0.05), jnp.log(2.0))
    example_factor = jnp.exp(log_factor)
    example_factor = example_factor.at[ranking[0]].set(2.0).at[ranking[1]].set(0.05)
    values = values * example_factor[None, :, None, None]
    return jnp.clip(values, -16.0, 16.0).astype(jnp.bfloat16)


def draw_lengths(key, part):
    length_key, ranking = example_order(key)
    values = jax.random.randint(length_key, (EXAMPLES,), SEQ // 8, SEQ + 1)
    values = values.at[ranking[0]].set(SEQ).at[ranking[1]].set(SEQ // 8)
    return values.astype(jnp.int32)


def setup_inputs(seed: int = 0) -> dict:
    keys = jax.random.split(jax.random.key(seed), 4)
    return {
        "activations": draw_activations(jax.random.fold_in(keys[3], 71), 0),
        "out_grads": draw_out_grads(jax.random.fold_in(keys[3], 71), 0),
        "lengths": draw_lengths(jax.random.fold_in(keys[3], 71), 0),
    }


def example_norm(operands):
    example_acts, example_grads = operands
    act_rows = example_acts.astype(jnp.float32)
    grad_values = example_grads.astype(jnp.float32)
    act_gram = jnp.dot(act_rows, act_rows.T, precision=lax.Precision.HIGHEST)
    grad_gram = jnp.dot(grad_values, grad_values.T, precision=lax.Precision.HIGHEST)
    return jnp.sum(act_gram * grad_gram)

def layer_norm_list(operands):
    return lax.map(example_norm, operands)

def reference(activations, out_grads, lengths):
    clip_bound = 0.5 * math.sqrt(float(LAYERS * SEQ * D * KV))
    positions = jnp.arange(SEQ, dtype=jnp.int32)
    token_keep = (positions[None, :] < lengths[:, None]).astype(jnp.bfloat16)
    masked = out_grads * token_keep[None, :, :, None]
    layer_norms = lax.map(layer_norm_list, (activations, masked))
    norm_total = lax.optimization_barrier(jnp.sum(layer_norms, axis=0))
    norm_ratio = jnp.sqrt(norm_total) / clip_bound
    clip_factor = 1.0 / jnp.maximum(norm_ratio, 1.0)

    def layer_grad(operands):
        layer_acts, layer_grads = operands
        scaled = (clip_factor[:, None, None] * layer_grads).astype(jnp.bfloat16)
        act_groups = layer_acts.reshape(N_DP, EX_DEV * SEQ, D)
        scaled_groups = scaled.reshape(N_DP, EX_DEV * SEQ, KV)

        def add_group(running, group):
            group_acts, group_scaled = group
            partial_sum = lax.dot_general(group_acts, group_scaled, (((0,), (0,)), ((), ())), preferred_element_type=jnp.float32)
            partial_sum = partial_sum.astype(jnp.bfloat16)
            return (running + partial_sum.astype(jnp.float32), None)
        summed, _ = lax.scan(add_group, jnp.zeros((D, KV), jnp.float32), (act_groups, scaled_groups))
        return (summed / EXAMPLES).astype(jnp.bfloat16)
    mean_grad = lax.map(layer_grad, (activations, masked))
    return (mean_grad, norm_ratio)
```

```python
import functools
import math

import jax
import jax.numpy as jnp
from jax import lax
from jax.experimental import pallas as pl
from jax.experimental.pallas import tpu as pltpu
from jax.sharding import PartitionSpec as P

MESH = pl.DeviceIdType.MESH
F32 = jnp.float32


def gram(rows, others):
    return lax.dot_general(rows, others, (((1,), (1,)), ((), ())), preferred_element_type=F32)


def kernel(
    plan,
    lengths_ref,
    acts_hbm,
    grads_hbm,
    out_ref,
    ratio_ref,
    acts,
    grads,
    norm_mine,
    norm_slots,
    pair_out,
    pair_in,
    line_out,
    line_in,
    load_sems,
    norm_send,
    norm_recv,
    pair_send,
    pair_recv,
    line_send,
    line_recv,
):
    examples, seq, outer, inner, sections, rows, subs, bound, examples_all = plan
    width = acts.shape[1]
    block = rows * subs
    place = lax.axis_index("dp")
    section = lax.axis_index("section")
    across = lax.rem(place, inner)
    along = lax.div(place, inner)
    partner = along * inner + (inner - 1 - across)

    loads = []
    for e in range(examples):
        span = pl.ds(e * seq, seq)
        copy = pltpu.make_async_copy(grads_hbm.at[span], grads.at[span], load_sems.at[e])
        copy.start()
        loads.append(copy)
    for e in range(examples):
        span = pl.ds(e * seq, seq)
        copy = pltpu.make_async_copy(
            acts_hbm.at[span], acts.at[span], load_sems.at[examples + e]
        )
        copy.start()
        loads.append(copy)

    barrier = pltpu.get_barrier_semaphore()
    for step in range(1, sections):
        peer = lax.rem(section + step, sections)
        pl.semaphore_signal(barrier, inc=1, device_id={"section": peer}, device_id_type=MESH)
    pl.semaphore_signal(barrier, inc=1, device_id={"dp": partner}, device_id_type=MESH)
    for step in range(1, outer):
        peer = lax.rem(along + step, outer) * inner + across
        pl.semaphore_signal(barrier, inc=1, device_id={"dp": peer}, device_id_type=MESH)

    half = seq // 2
    tile_row = lax.broadcasted_iota(jnp.int32, norm_mine.shape, 0)
    mine = jnp.zeros(norm_mine.shape, F32)
    for e in range(examples):
        base = e * seq
        span = pl.ds(base, seq)
        top, bottom = pl.ds(base, half), pl.ds(base + half, half)
        loads[e].wait()
        token = lax.broadcasted_iota(jnp.int32, (seq, grads.shape[1]), 0)
        keep = (token < lengths_ref[e]).astype(F32)
        grads[span] = (grads[span].astype(F32) * keep).astype(jnp.bfloat16)
        grad_top = gram(grads[top], grads[span])
        grad_low = gram(grads[bottom], grads[bottom])
        loads[examples + e].wait()
        prod_top = gram(acts[top], acts[span]) * grad_top
        prod_low = gram(acts[bottom], acts[bottom]) * grad_low
        norm = (
            jnp.sum(prod_top[:, :half])
            + 2.0 * jnp.sum(prod_top[:, half:])
            + jnp.sum(prod_low)
        )
        mine = jnp.where(tile_row == e, norm, mine)
    norm_mine[...] = mine
    norm_slots[section] = mine

    pl.semaphore_wait(barrier, sections - 1 + 1 + outer - 1)

    norm_copies = []
    for step in range(1, sections):
        peer = lax.rem(section + step, sections)
        copy = pltpu.make_async_remote_copy(
            src_ref=norm_mine,
            dst_ref=norm_slots.at[section],
            send_sem=norm_send.at[step],
            recv_sem=norm_recv.at[step],
            device_id={"section": peer},
            device_id_type=MESH,
        )
        copy.start()
        norm_copies.append(copy)
    for copy in norm_copies:
        copy.wait()
    total = norm_slots[0]
    for s in range(1, sections):
        total = total + norm_slots[s]
    ratio = jnp.sqrt(total) / bound
    ratio_ref[...] = ratio
    factor = 1.0 / jnp.maximum(ratio, 1.0)
    for e in range(examples):
        span = pl.ds(e * seq, seq)
        scale = factor[e : e + 1, 0:1]
        grads[span] = (grads[span].astype(F32) * scale).astype(jnp.bfloat16)

    def partial(line, side, sub):
        start = (line * inner + side) * block + sub * rows
        columns = pl.ds(pl.multiple_of(start, rows), rows)
        return lax.dot_general(
            acts[:, columns], grads[...], (((0,), (0,)), ((), ())), preferred_element_type=F32
        )

    def target(k):
        return lax.rem(along + 1 + lax.div(k, subs), outer), lax.rem(k, subs)

    def pair_copy(k):
        return pltpu.make_async_remote_copy(
            src_ref=pair_out.at[k],
            dst_ref=pair_in.at[k],
            send_sem=pair_send.at[k],
            recv_sem=pair_recv.at[k],
            device_id={"dp": partner},
            device_id_type=MESH,
        )

    def line_copy(k):
        line, sub = target(k)
        return pltpu.make_async_remote_copy(
            src_ref=line_out.at[k],
            dst_ref=line_in.at[k],
            send_sem=line_send.at[k],
            recv_sem=line_recv.at[k],
            device_id={"dp": line * inner + across},
            device_id_type=MESH,
        )

    chunks = outer * subs
    remote = (outer - 1) * subs

    @pl.loop(0, chunks)
    def _(k):
        line, sub = target(k)
        pair_out[k] = partial(line, inner - 1 - across, sub).astype(jnp.bfloat16)
        pair_copy(k).start()

    @pl.loop(0, remote)
    def _(k):
        line, sub = target(k)
        own = partial(line, across, sub)
        pair_copy(k).wait_recv()
        line_out[k] = (own + pair_in[k].astype(F32)).astype(jnp.bfloat16)
        line_copy(k).start()

    @pl.loop(0, subs)
    def _(sub):
        own = partial(along, across, sub)
        pair_copy(remote + sub).wait_recv()
        own = own + pair_in[remote + sub].astype(F32)
        for step in range(outer - 1):
            line_copy(step * subs + sub).wait_recv()
            own = own + line_in[step * subs + sub].astype(F32)
        into = pl.ds(pl.multiple_of(sub * rows, rows), rows)
        out_ref[into] = (own / examples_all).astype(jnp.bfloat16)

    @pl.loop(0, chunks)
    def _(k):
        pair_copy(k).wait_send()

    @pl.loop(0, remote)
    def _(k):
        line_copy(k).wait_send()


def on_device(sections, places, activations, out_grads, lengths):
    layers, examples, seq, width = activations.shape
    features = out_grads.shape[3]
    inner = 2
    outer = places // inner
    block = width // places
    rows = min(block, 128)
    subs = block // rows
    bound = 0.5 * math.sqrt(float(layers * sections * seq * width * features))
    plan = (examples, seq, outer, inner, sections, rows, subs, bound, float(places * examples))
    chunks = outer * subs
    remote = (outer - 1) * subs
    tokens = examples * seq
    tile = (max(8, -(-examples // 8) * 8), 128)
    dma = pltpu.SemaphoreType.DMA
    bf16 = jnp.bfloat16
    grad, ratio = pl.pallas_call(
        functools.partial(kernel, plan),
        out_shape=(
            jax.ShapeDtypeStruct((block, features), bf16),
            jax.ShapeDtypeStruct(tile, F32),
        ),
        in_specs=[
            pl.BlockSpec(memory_space=pltpu.SMEM),
            pl.BlockSpec(memory_space=pl.ANY),
            pl.BlockSpec(memory_space=pl.ANY),
        ],
        out_specs=(
            pl.BlockSpec(memory_space=pltpu.VMEM),
            pl.BlockSpec(memory_space=pltpu.VMEM),
        ),
        scratch_shapes=[
            pltpu.VMEM((tokens, width), bf16),
            pltpu.VMEM((tokens, features), bf16),
            pltpu.VMEM(tile, F32),
            pltpu.VMEM((sections,) + tile, F32),
            pltpu.VMEM((chunks, rows, features), bf16),
            pltpu.VMEM((chunks, rows, features), bf16),
            pltpu.VMEM((remote, rows, features), bf16),
            pltpu.VMEM((remote, rows, features), bf16),
            dma((2 * examples,)),
            dma((sections,)),
            dma((sections,)),
            dma((chunks,)),
            dma((chunks,)),
            dma((remote,)),
            dma((remote,)),
        ],
        compiler_params=pltpu.CompilerParams(
            collective_id=0, has_side_effects=True, vmem_limit_bytes=56 * 2**20
        ),
    )(
        lengths,
        activations.reshape(tokens, width),
        out_grads.reshape(tokens, features),
    )
    return grad[None], ratio[:examples, 0]


def solution(mesh):
    placed = (P("section", "dp", None, None), P("section", "dp", None, None), P("dp"))
    return jax.shard_map(
        functools.partial(on_device, mesh.shape["section"], mesh.shape["dp"]),
        mesh=mesh,
        in_specs=placed,
        out_specs=(P("section", "dp", None), P("dp")),
        check_vma=False,
    )
```

```python
import functools
import math

import jax
import jax.numpy as jnp
from jax import lax
from jax.experimental import pallas as pl
from jax.experimental.pallas import tpu as pltpu
from jax.sharding import PartitionSpec as P

MESH = pl.DeviceIdType.MESH
F32 = jnp.float32


def gram(rows, others):
    return lax.dot_general(rows, others, (((1,), (1,)), ((), ())), preferred_element_type=F32)


def kernel(
    plan,
    lengths_ref,
    acts_hbm,
    grads_hbm,
    out_ref,
    ratio_ref,
    acts,
    grads,
    norm_mine,
    norm_slots,
    pair_out,
    pair_in,
    line_out,
    line_in,
    load_sems,
    norm_send,
    norm_recv,
    pair_send,
    pair_recv,
    line_send,
    line_recv,
):
    examples, seq, outer, inner, sections, rows, subs, bound, examples_all = plan
    width = acts.shape[1]
    block = rows * subs
    place = lax.axis_index("dp")
    section = lax.axis_index("section")
    across = lax.rem(place, inner)
    along = lax.div(place, inner)
    partner = along * inner + (inner - 1 - across)

    loads = []
    for e in range(examples):
        span = pl.ds(e * seq, seq)
        copy = pltpu.make_async_copy(grads_hbm.at[span], grads.at[span], load_sems.at[e])
        copy.start()
        loads.append(copy)
    for e in range(examples):
        span = pl.ds(e * seq, seq)
        copy = pltpu.make_async_copy(
            acts_hbm.at[span], acts.at[span], load_sems.at[examples + e]
        )
        copy.start()
        loads.append(copy)

    barrier = pltpu.get_barrier_semaphore()
    for step in range(1, sections):
        peer = lax.rem(section + step, sections)
        pl.semaphore_signal(barrier, inc=1, device_id={"section": peer}, device_id_type=MESH)
    pl.semaphore_signal(barrier, inc=1, device_id={"dp": partner}, device_id_type=MESH)
    for step in range(1, outer):
        peer = lax.rem(along + step, outer) * inner + across
        pl.semaphore_signal(barrier, inc=1, device_id={"dp": peer}, device_id_type=MESH)

    half = seq // 2
    tile_row = lax.broadcasted_iota(jnp.int32, norm_mine.shape, 0)
    mine = jnp.zeros(norm_mine.shape, F32)
    for e in range(examples):
        base = e * seq
        span = pl.ds(base, seq)
        top, bottom = pl.ds(base, half), pl.ds(base + half, half)
        loads[e].wait()
        token = lax.broadcasted_iota(jnp.int32, (seq, grads.shape[1]), 0)
        keep = (token < lengths_ref[e]).astype(F32)
        grads[span] = (grads[span].astype(F32) * keep).astype(jnp.bfloat16)
        grad_top = gram(grads[top], grads[span])
        grad_low = gram(grads[bottom], grads[bottom])
        loads[examples + e].wait()
        prod_top = gram(acts[top], acts[span]) * grad_top
        prod_low = gram(acts[bottom], acts[bottom]) * grad_low
        norm = (
            jnp.sum(prod_top[:, :half])
            + 2.0 * jnp.sum(prod_top[:, half:])
            + jnp.sum(prod_low)
        )
        mine = jnp.where(tile_row == e, norm, mine)
    norm_mine[...] = mine
    norm_slots[section] = mine

    pl.semaphore_wait(barrier, sections - 1 + 1 + outer - 1)

    norm_copies = []
    for step in range(1, sections):
        peer = lax.rem(section + step, sections)
        copy = pltpu.make_async_remote_copy(
            src_ref=norm_mine,
            dst_ref=norm_slots.at[section],
            send_sem=norm_send.at[step],
            recv_sem=norm_recv.at[step],
            device_id={"section": peer},
            device_id_type=MESH,
        )
        copy.start()
        norm_copies.append(copy)
    for copy in norm_copies:
        copy.wait()
    total = norm_slots[0]
    for s in range(1, sections):
        total = total + norm_slots[s]
    ratio = jnp.sqrt(total) / bound
    first_column = lax.broadcasted_iota(jnp.int32, norm_mine.shape, 1) == 0
    for e in range(examples):
        chosen = jnp.logical_and(tile_row == e, first_column)
        ratio_ref[e] = jnp.sum(jnp.where(chosen, ratio, 0.0))
    factor = 1.0 / jnp.maximum(ratio, 1.0)
    for e in range(examples):
        span = pl.ds(e * seq, seq)
        scale = factor[e : e + 1, 0:1]
        grads[span] = (grads[span].astype(F32) * scale).astype(jnp.bfloat16)

    def partial(line, side, sub):
        start = (line * inner + side) * block + sub * rows
        columns = pl.ds(pl.multiple_of(start, rows), rows)
        return lax.dot_general(
            acts[:, columns], grads[...], (((0,), (0,)), ((), ())), preferred_element_type=F32
        )

    relayed = outer == 4
    far_half = lax.div(along, 2)
    at_end = jnp.logical_or(along == 0, along == outer - 1)

    def target(k):
        turn, sub = lax.div(k, subs), lax.rem(k, subs)
        if not relayed:
            return lax.rem(along + 1 + turn, outer), sub
        mirrored = jnp.where(far_half == 1, outer - 1 - along, along)
        line = lax.rem(outer - 1 + mirrored - turn + outer, outer)
        return jnp.where(far_half == 1, outer - 1 - line, line), sub

    def pair_copy(k):
        return pltpu.make_async_remote_copy(
            src_ref=pair_out.at[k],
            dst_ref=pair_in.at[k],
            send_sem=pair_send.at[k],
            recv_sem=pair_recv.at[k],
            device_id={"dp": partner},
            device_id_type=MESH,
        )

    def landing(k, slot, line):
        return pltpu.make_async_remote_copy(
            src_ref=line_out.at[k],
            dst_ref=line_in.at[slot],
            send_sem=line_send.at[k],
            recv_sem=line_recv.at[slot],
            device_id={"dp": line * inner + across},
            device_id_type=MESH,
        )

    def crosses(line):
        return lax.div(line, 2) != far_half

    def line_copy(k):
        line, sub = target(k)
        if not relayed:
            return landing(k, k, line)
        handed = jnp.logical_and(at_end, crosses(line))
        direct = jnp.where(crosses(line), 1, 0)
        slot = jnp.where(handed, 2 + lax.rem(line, 2), direct)
        stop = jnp.where(at_end, jnp.where(along == 0, 1, outer - 2), line)
        return landing(k, slot * subs + sub, stop)

    chunks = outer * subs
    remote = (outer - 1) * subs

    @pl.loop(0, chunks)
    def _(k):
        line, sub = target(k)
        pair_out[k] = partial(line, inner - 1 - across, sub).astype(jnp.bfloat16)
        pair_copy(k).start()

    @pl.loop(0, remote)
    def _(k):
        line, sub = target(k)
        own = partial(line, across, sub)
        pair_copy(k).wait_recv()
        own = own + pair_in[k].astype(F32)
        if relayed:
            adds = jnp.logical_and(jnp.logical_not(at_end), crosses(line))

            @pl.when(adds)
            def _():
                slot = (2 + lax.rem(line, 2)) * subs + sub
                landing(k, slot, line).wait_recv()
                line_out[k] = (own + line_in[slot].astype(F32)).astype(jnp.bfloat16)

            @pl.when(jnp.logical_not(adds))
            def _():
                line_out[k] = own.astype(jnp.bfloat16)

        else:
            line_out[k] = own.astype(jnp.bfloat16)
        line_copy(k).start()

    @pl.loop(0, subs)
    def _(sub):
        own = partial(along, across, sub)
        pair_copy(remote + sub).wait_recv()
        own = own + pair_in[remote + sub].astype(F32)
        for step in range(2 if relayed else outer - 1):
            slot = step * subs + sub
            landing(slot, slot, along).wait_recv()
            own = own + line_in[slot].astype(F32)
        into = pl.ds(pl.multiple_of(sub * rows, rows), rows)
        out_ref[into] = (own / examples_all).astype(jnp.bfloat16)

    @pl.loop(0, chunks)
    def _(k):
        pair_copy(k).wait_send()

    @pl.loop(0, remote)
    def _(k):
        line_copy(k).wait_send()


def on_device(sections, places, activations, out_grads, lengths):
    layers, examples, seq, width = activations.shape
    features = out_grads.shape[3]
    inner = 2
    outer = places // inner
    block = width // places
    rows = min(block, 128)
    subs = block // rows
    bound = 0.5 * math.sqrt(float(layers * sections * seq * width * features))
    plan = (examples, seq, outer, inner, sections, rows, subs, bound, float(places * examples))
    chunks = outer * subs
    remote = (outer - 1) * subs
    tokens = examples * seq
    tile = (max(8, -(-examples // 8) * 8), 128)
    dma = pltpu.SemaphoreType.DMA
    bf16 = jnp.bfloat16
    grad, ratio = pl.pallas_call(
        functools.partial(kernel, plan),
        out_shape=(
            jax.ShapeDtypeStruct((block, features), bf16),
            jax.ShapeDtypeStruct((examples,), F32),
        ),
        in_specs=[
            pl.BlockSpec(memory_space=pltpu.SMEM),
            pl.BlockSpec(memory_space=pl.ANY),
            pl.BlockSpec(memory_space=pl.ANY),
        ],
        out_specs=(
            pl.BlockSpec(memory_space=pltpu.VMEM),
            pl.BlockSpec(memory_space=pltpu.SMEM),
        ),
        scratch_shapes=[
            pltpu.VMEM((tokens, width), bf16),
            pltpu.VMEM((tokens, features), bf16),
            pltpu.VMEM(tile, F32),
            pltpu.VMEM((sections,) + tile, F32),
            pltpu.VMEM((chunks, rows, features), bf16),
            pltpu.VMEM((chunks, rows, features), bf16),
            pltpu.VMEM((remote, rows, features), bf16),
            pltpu.VMEM((chunks, rows, features), bf16),
            dma((2 * examples,)),
            dma((sections,)),
            dma((sections,)),
            dma((chunks,)),
            dma((chunks,)),
            dma((remote,)),
            dma((chunks,)),
        ],
        compiler_params=pltpu.CompilerParams(
            collective_id=0, has_side_effects=True, vmem_limit_bytes=56 * 2**20
        ),
    )(
        lengths,
        activations.reshape(tokens, width),
        out_grads.reshape(tokens, features),
    )
    return grad[None], ratio


def solution(mesh):
    placed = (P("section", "dp", None, None), P("section", "dp", None, None), P("dp"))
    return jax.shard_map(
        functools.partial(on_device, mesh.shape["section"], mesh.shape["dp"]),
        mesh=mesh,
        in_specs=placed,
        out_specs=(P("section", "dp", None), P("dp")),
        check_vma=False,
    )
```

```python
import functools
import math

import jax
import jax.numpy as jnp
from jax import lax
from jax.experimental import pallas as pl
from jax.experimental.pallas import tpu as pltpu
from jax.sharding import PartitionSpec as P

MESH = pl.DeviceIdType.MESH
F32 = jnp.float32


def gram(rows, others):
    return lax.dot_general(rows, others, (((1,), (1,)), ((), ())), preferred_element_type=F32)


def kernel(
    plan,
    lengths_ref,
    acts_hbm,
    grads_hbm,
    out_ref,
    ratio_ref,
    acts,
    grads,
    norm_mine,
    norm_slots,
    pair_out,
    pair_in,
    line_out,
    line_in,
    late_out,
    late_in,
    total_ref,
    load_sems,
    norm_send,
    norm_recv,
    pair_send,
    pair_recv,
    line_send,
    line_recv,
    late_send,
    late_recv,
):
    examples, seq, outer, inner, sections, rows, subs, bound, examples_all = plan
    width = acts.shape[1]
    block = rows * subs
    place = lax.axis_index("dp")
    section = lax.axis_index("section")
    across = lax.rem(place, inner)
    along = lax.div(place, inner)
    partner = along * inner + (inner - 1 - across)

    loads = []
    for e in range(examples):
        span = pl.ds(e * seq, seq)
        copy = pltpu.make_async_copy(grads_hbm.at[span], grads.at[span], load_sems.at[e])
        copy.start()
        loads.append(copy)
    for e in range(examples):
        span = pl.ds(e * seq, seq)
        copy = pltpu.make_async_copy(
            acts_hbm.at[span], acts.at[span], load_sems.at[examples + e]
        )
        copy.start()
        loads.append(copy)

    barrier = pltpu.get_barrier_semaphore()
    for step in range(1, sections):
        peer = lax.rem(section + step, sections)
        pl.semaphore_signal(barrier, inc=1, device_id={"section": peer}, device_id_type=MESH)
    pl.semaphore_signal(barrier, inc=1, device_id={"dp": partner}, device_id_type=MESH)
    for step in range(1, outer):
        peer = lax.rem(along + step, outer) * inner + across
        pl.semaphore_signal(barrier, inc=1, device_id={"dp": peer}, device_id_type=MESH)

    half = seq // 2
    tile_row = lax.broadcasted_iota(jnp.int32, norm_mine.shape, 0)
    mine = jnp.zeros(norm_mine.shape, F32)
    for e in range(examples):
        base = e * seq
        span = pl.ds(base, seq)
        top, bottom = pl.ds(base, half), pl.ds(base + half, half)
        loads[e].wait()
        token = lax.broadcasted_iota(jnp.int32, (seq, grads.shape[1]), 0)
        keep = (token < lengths_ref[e]).astype(F32)
        grads[span] = (grads[span].astype(F32) * keep).astype(jnp.bfloat16)
        grad_top = gram(grads[top], grads[span])
        grad_low = gram(grads[bottom], grads[bottom])
        loads[examples + e].wait()
        prod_top = gram(acts[top], acts[span]) * grad_top
        prod_low = gram(acts[bottom], acts[bottom]) * grad_low
        norm = (
            jnp.sum(prod_top[:, :half])
            + 2.0 * jnp.sum(prod_top[:, half:])
            + jnp.sum(prod_low)
        )
        mine = jnp.where(tile_row == e, norm, mine)
    norm_mine[...] = mine
    norm_slots[section] = mine

    pl.semaphore_wait(barrier, sections - 1 + 1 + outer - 1)

    norm_copies = []
    for step in range(1, sections):
        peer = lax.rem(section + step, sections)
        copy = pltpu.make_async_remote_copy(
            src_ref=norm_mine,
            dst_ref=norm_slots.at[section],
            send_sem=norm_send.at[step],
            recv_sem=norm_recv.at[step],
            device_id={"section": peer},
            device_id_type=MESH,
        )
        copy.start()
        norm_copies.append(copy)
    for copy in norm_copies:
        copy.wait()
    total = norm_slots[0]
    for s in range(1, sections):
        total = total + norm_slots[s]
    ratio = jnp.sqrt(total) / bound
    first_column = lax.broadcasted_iota(jnp.int32, norm_mine.shape, 1) == 0
    for e in range(examples):
        chosen = jnp.logical_and(tile_row == e, first_column)
        ratio_ref[e] = jnp.sum(jnp.where(chosen, ratio, 0.0))
    factor = 1.0 / jnp.maximum(ratio, 1.0)
    for e in range(examples):
        span = pl.ds(e * seq, seq)
        scale = factor[e : e + 1, 0:1]
        grads[span] = (grads[span].astype(F32) * scale).astype(jnp.bfloat16)

    def partial(line, side, sub):
        start = (line * inner + side) * block + sub * rows
        columns = pl.ds(pl.multiple_of(start, rows), rows)
        return lax.dot_general(
            acts[:, columns], grads[...], (((0,), (0,)), ((), ())), preferred_element_type=F32
        )

    relayed = outer == 4
    far_half = lax.div(along, 2)
    at_end = jnp.logical_or(along == 0, along == outer - 1)

    def target(k):
        turn, sub = lax.div(k, subs), lax.rem(k, subs)
        if not relayed:
            return lax.rem(along + 1 + turn, outer), sub
        mirrored = jnp.where(far_half == 1, outer - 1 - along, along)
        line = lax.rem(outer - 1 + mirrored - turn + outer, outer)
        return jnp.where(far_half == 1, outer - 1 - line, line), sub

    def pair_copy(k):
        return pltpu.make_async_remote_copy(
            src_ref=pair_out.at[k],
            dst_ref=pair_in.at[k],
            send_sem=pair_send.at[k],
            recv_sem=pair_recv.at[k],
            device_id={"dp": partner},
            device_id_type=MESH,
        )

    def copy_along(bufs, k, slot, line):
        source, land, send, recv = bufs
        return pltpu.make_async_remote_copy(
            src_ref=source.at[k],
            dst_ref=land.at[slot],
            send_sem=send.at[k],
            recv_sem=recv.at[slot],
            device_id={"dp": line * inner + across},
            device_id_type=MESH,
        )

    landing = functools.partial(copy_along, (line_out, line_in, line_send, line_recv))
    late_landing = functools.partial(copy_along, (late_out, late_in, late_send, late_recv))

    def crosses(line):
        return lax.div(line, 2) != far_half

    def adds(line):
        return jnp.logical_and(jnp.logical_not(at_end), crosses(line))

    def route(line):
        handed = jnp.logical_and(at_end, crosses(line))
        direct = jnp.where(crosses(line), 1, 0)
        slot = jnp.where(handed, 2 + lax.rem(line, 2), direct)
        stop = jnp.where(at_end, jnp.where(along == 0, 1, outer - 2), line)
        return slot, stop

    def line_copy(k):
        line, sub = target(k)
        if not relayed:
            return landing(k, k, line)
        slot, stop = route(line)
        return landing(k, slot * subs + sub, stop)

    def late_copy(turn, line):
        slot, stop = route(line)
        return late_landing(turn, slot, stop)

    def late_line(line):
        return line != 2

    def is_late(line, sub):
        if not relayed:
            return jnp.bool_(False)
        return jnp.logical_and(sub == subs - 1, late_line(line))

    chunks = outer * subs
    remote = (outer - 1) * subs

    def exchange(k):
        line, sub = target(k)

        @pl.when(jnp.logical_not(is_late(line, sub)))
        def _():
            pair_out[k] = partial(line, inner - 1 - across, sub).astype(jnp.bfloat16)
            pair_copy(k).start()

    def late(turn):
        line, _ = target(turn * subs)

        @pl.when(late_line(line))
        def _():
            total_ref[...] = partial(line, inner - 1 - across, subs - 1)

            @pl.when(adds(line))
            def _():
                slot = 2 + lax.rem(line, 2)
                late_landing(turn, slot, line).wait_recv()
                total_ref[...] += late_in[slot].astype(F32)

            late_out[turn] = total_ref[...].astype(jnp.bfloat16)
            late_copy(turn, line).start()

    pl.loop(0, 1)(exchange)
    if relayed:
        pl.loop(0, 1)(late)
    pl.loop(1, chunks)(exchange)
    if relayed:
        pl.loop(1, outer - 1)(late)

    def forward(k):
        line, sub = target(k)
        total_ref[...] = partial(line, across, sub)

        @pl.when(jnp.logical_not(is_late(line, sub)))
        def _():
            pair_copy(k).wait_recv()
            total_ref[...] += pair_in[k].astype(F32)

        if relayed:

            @pl.when(adds(line))
            def _():
                slot = (2 + lax.rem(line, 2)) * subs + sub
                landing(k, slot, line).wait_recv()
                total_ref[...] += line_in[slot].astype(F32)

        line_out[k] = total_ref[...].astype(jnp.bfloat16)
        line_copy(k).start()

    pl.loop(0, subs)(forward)

    if relayed:

        @pl.when(late_line(along))
        def _():
            own = partial(along, inner - 1 - across, subs - 1)
            for slot in range(2):
                late_landing(slot, slot, along).wait_recv()
                own = own + late_in[slot].astype(F32)
            pair_out[chunks - 1] = own.astype(jnp.bfloat16)
            pair_copy(chunks - 1).start()

    pl.loop(subs, remote)(forward)

    @pl.loop(0, subs)
    def _(sub):
        own = partial(along, across, sub)
        pair_copy(remote + sub).wait_recv()
        own = own + pair_in[remote + sub].astype(F32)
        for step in range(2 if relayed else outer - 1):
            slot = step * subs + sub
            landing(slot, slot, along).wait_recv()
            own = own + line_in[slot].astype(F32)
        into = pl.ds(pl.multiple_of(sub * rows, rows), rows)
        out_ref[into] = (own / examples_all).astype(jnp.bfloat16)

    @pl.loop(0, chunks)
    def _(k):
        line, sub = target(k)

        @pl.when(jnp.logical_not(jnp.logical_and(is_late(line, sub), k < remote)))
        def _():
            pair_copy(k).wait_send()

    if relayed:

        @pl.loop(0, outer - 1)
        def _(turn):
            line, _ = target(turn * subs)

            @pl.when(late_line(line))
            def _():
                late_copy(turn, line).wait_send()

    @pl.loop(0, remote)
    def _(k):
        line_copy(k).wait_send()


def on_device(sections, places, activations, out_grads, lengths):
    layers, examples, seq, width = activations.shape
    features = out_grads.shape[3]
    inner = 2
    outer = places // inner
    block = width // places
    rows = min(block, 128)
    subs = block // rows
    bound = 0.5 * math.sqrt(float(layers * sections * seq * width * features))
    plan = (examples, seq, outer, inner, sections, rows, subs, bound, float(places * examples))
    chunks = outer * subs
    remote = (outer - 1) * subs
    tokens = examples * seq
    tile = (max(8, -(-examples // 8) * 8), 128)
    dma = pltpu.SemaphoreType.DMA
    bf16 = jnp.bfloat16
    grad, ratio = pl.pallas_call(
        functools.partial(kernel, plan),
        out_shape=(
            jax.ShapeDtypeStruct((block, features), bf16),
            jax.ShapeDtypeStruct((examples,), F32),
        ),
        in_specs=[
            pl.BlockSpec(memory_space=pltpu.SMEM),
            pl.BlockSpec(memory_space=pl.ANY),
            pl.BlockSpec(memory_space=pl.ANY),
        ],
        out_specs=(
            pl.BlockSpec(memory_space=pltpu.VMEM),
            pl.BlockSpec(memory_space=pltpu.SMEM),
        ),
        scratch_shapes=[
            pltpu.VMEM((tokens, width), bf16),
            pltpu.VMEM((tokens, features), bf16),
            pltpu.VMEM(tile, F32),
            pltpu.VMEM((sections,) + tile, F32),
            pltpu.VMEM((chunks, rows, features), bf16),
            pltpu.VMEM((chunks, rows, features), bf16),
            pltpu.VMEM((remote, rows, features), bf16),
            pltpu.VMEM((chunks, rows, features), bf16),
            pltpu.VMEM((outer - 1, rows, features), bf16),
            pltpu.VMEM((4, rows, features), bf16),
            pltpu.VMEM((rows, features), F32),
            dma((2 * examples,)),
            dma((sections,)),
            dma((sections,)),
            dma((chunks,)),
            dma((chunks,)),
            dma((remote,)),
            dma((chunks,)),
            dma((outer - 1,)),
            dma((4,)),
        ],
        compiler_params=pltpu.CompilerParams(
            collective_id=0, has_side_effects=True, vmem_limit_bytes=56 * 2**20
        ),
    )(
        lengths,
        activations.reshape(tokens, width),
        out_grads.reshape(tokens, features),
    )
    return grad[None], ratio


def solution(mesh):
    placed = (P("section", "dp", None, None), P("section", "dp", None, None), P("dp"))
    return jax.shard_map(
        functools.partial(on_device, mesh.shape["section"], mesh.shape["dp"]),
        mesh=mesh,
        in_specs=placed,
        out_specs=(P("section", "dp", None), P("dp")),
        check_vma=False,
    )
```

```python
import functools
import math

import jax
import jax.numpy as jnp
from jax import lax
from jax.experimental import pallas as pl
from jax.experimental.pallas import tpu as pltpu
from jax.sharding import PartitionSpec as P

MESH = pl.DeviceIdType.MESH
F32 = jnp.float32


def gram(rows, others):
    return lax.dot_general(rows, others, (((1,), (1,)), ((), ())), preferred_element_type=F32)


def kernel(
    plan,
    lengths_ref,
    acts_hbm,
    grads_hbm,
    out_ref,
    ratio_ref,
    acts,
    grads,
    norm_mine,
    norm_slots,
    pair_out,
    pair_in,
    line_out,
    line_in,
    late_out,
    late_in,
    total_ref,
    load_sems,
    norm_send,
    norm_recv,
    pair_send,
    pair_recv,
    line_send,
    line_recv,
    late_send,
    late_recv,
):
    examples, seq, outer, inner, sections, rows, subs, bound, examples_all = plan
    width = acts.shape[1]
    block = rows * subs
    place = lax.axis_index("dp")
    section = lax.axis_index("section")
    across = lax.rem(place, inner)
    along = lax.div(place, inner)
    partner = along * inner + (inner - 1 - across)

    loads = []
    for e in range(examples):
        span = pl.ds(e * seq, seq)
        copy = pltpu.make_async_copy(grads_hbm.at[span], grads.at[span], load_sems.at[e])
        copy.start()
        more = pltpu.make_async_copy(
            acts_hbm.at[span], acts.at[span], load_sems.at[examples + e]
        )
        more.start()
        loads.append((copy, more))

    barrier = pltpu.get_barrier_semaphore()
    for step in range(1, sections):
        peer = lax.rem(section + step, sections)
        pl.semaphore_signal(barrier, inc=1, device_id={"section": peer}, device_id_type=MESH)
    pl.semaphore_signal(barrier, inc=1, device_id={"dp": partner}, device_id_type=MESH)
    for step in range(1, outer):
        peer = lax.rem(along + step, outer) * inner + across
        pl.semaphore_signal(barrier, inc=1, device_id={"dp": peer}, device_id_type=MESH)

    half = seq // 2
    tile_row = lax.broadcasted_iota(jnp.int32, norm_mine.shape, 0)
    mine = jnp.zeros(norm_mine.shape, F32)
    for e in range(examples):
        base = e * seq
        span = pl.ds(base, seq)
        top, bottom = pl.ds(base, half), pl.ds(base + half, half)
        grads_load, acts_load = loads[e]
        grads_load.wait()
        grad_top = gram(grads[top], grads[span])
        grad_low = gram(grads[bottom], grads[bottom])
        acts_load.wait()
        prod_top = gram(acts[top], acts[span]) * grad_top
        prod_low = gram(acts[bottom], acts[bottom]) * grad_low
        length = lengths_ref[e]
        at_row = lax.broadcasted_iota(jnp.int32, (half, half), 0)
        at_col = lax.broadcasted_iota(jnp.int32, (half, half), 1)
        latest = jnp.maximum(at_row, at_col)
        entries = jnp.where(latest < length, prod_top[:, :half], 0.0)
        entries += jnp.where(
            jnp.logical_and(at_row < length, at_col + half < length),
            2.0 * prod_top[:, half:],
            0.0,
        )
        entries += jnp.where(latest + half < length, prod_low, 0.0)
        norm = jnp.sum(entries, keepdims=True)
        mine = jnp.where(tile_row == e, norm, mine)
    norm_mine[...] = mine
    norm_slots[section] = mine

    pl.semaphore_wait(barrier, sections - 1 + 1 + outer - 1)

    norm_copies = []
    for step in range(1, sections):
        peer = lax.rem(section + step, sections)
        copy = pltpu.make_async_remote_copy(
            src_ref=norm_mine,
            dst_ref=norm_slots.at[section],
            send_sem=norm_send.at[step],
            recv_sem=norm_recv.at[step],
            device_id={"section": peer},
            device_id_type=MESH,
        )
        copy.start()
        norm_copies.append(copy)
    for copy in norm_copies:
        copy.wait()
    total = norm_slots[0]
    for s in range(1, sections):
        total = total + norm_slots[s]
    ratio = jnp.sqrt(total) / bound
    factor = 1.0 / jnp.maximum(ratio, 1.0)
    for e in range(examples):
        span = pl.ds(e * seq, seq)
        token = lax.broadcasted_iota(jnp.int32, (seq, 1), 0)
        scale = jnp.where(token < lengths_ref[e], factor[e : e + 1, 0:1], 0.0)
        grads[span] = (grads[span].astype(F32) * scale).astype(jnp.bfloat16)

    def partial(line, side, sub):
        start = (line * inner + side) * block + sub * rows
        columns = pl.ds(pl.multiple_of(start, rows), rows)
        return lax.dot_general(
            acts[:, columns], grads[...], (((0,), (0,)), ((), ())), preferred_element_type=F32
        )

    relayed = outer == 4
    far_half = lax.div(along, 2)
    at_end = jnp.logical_or(along == 0, along == outer - 1)

    def target(k):
        turn, sub = lax.div(k, subs), lax.rem(k, subs)
        if not relayed:
            return lax.rem(along + 1 + turn, outer), sub
        mirrored = jnp.where(far_half == 1, outer - 1 - along, along)
        line = lax.rem(outer - 1 + mirrored - turn + outer, outer)
        return jnp.where(far_half == 1, outer - 1 - line, line), sub

    def pair_copy(k):
        return pltpu.make_async_remote_copy(
            src_ref=pair_out.at[k],
            dst_ref=pair_in.at[k],
            send_sem=pair_send.at[k],
            recv_sem=pair_recv.at[k],
            device_id={"dp": partner},
            device_id_type=MESH,
        )

    def copy_along(bufs, k, slot, line):
        source, land, send, recv = bufs
        return pltpu.make_async_remote_copy(
            src_ref=source.at[k],
            dst_ref=land.at[slot],
            send_sem=send.at[k],
            recv_sem=recv.at[slot],
            device_id={"dp": line * inner + across},
            device_id_type=MESH,
        )

    landing = functools.partial(copy_along, (line_out, line_in, line_send, line_recv))
    late_landing = functools.partial(copy_along, (late_out, late_in, late_send, late_recv))

    def crosses(line):
        return lax.div(line, 2) != far_half

    def adds(line):
        return jnp.logical_and(jnp.logical_not(at_end), crosses(line))

    def route(line):
        handed = jnp.logical_and(at_end, crosses(line))
        direct = jnp.where(crosses(line), 1, 0)
        slot = jnp.where(handed, 2 + lax.rem(line, 2), direct)
        stop = jnp.where(at_end, jnp.where(along == 0, 1, outer - 2), line)
        return slot, stop

    def line_copy(k):
        line, sub = target(k)
        if not relayed:
            return landing(k, k, line)
        slot, stop = route(line)
        return landing(k, slot * subs + sub, stop)

    def late_copy(turn, line):
        slot, stop = route(line)
        return late_landing(turn, slot, stop)

    def late_line(line):
        return line != 2

    def is_late(line, sub):
        if not relayed:
            return jnp.bool_(False)
        return jnp.logical_and(sub == subs - 1, late_line(line))

    chunks = outer * subs
    remote = (outer - 1) * subs

    def exchange(k):
        line, sub = target(k)

        @pl.when(jnp.logical_not(is_late(line, sub)))
        def _():
            pair_out[k] = partial(line, inner - 1 - across, sub).astype(jnp.bfloat16)
            pair_copy(k).start()

    def late(turn):
        line, _ = target(turn * subs)

        @pl.when(late_line(line))
        def _():
            total_ref[...] = partial(line, inner - 1 - across, subs - 1)

            @pl.when(adds(line))
            def _():
                slot = 2 + lax.rem(line, 2)
                late_landing(turn, slot, line).wait_recv()
                total_ref[...] += late_in[slot].astype(F32)

            late_out[turn] = total_ref[...].astype(jnp.bfloat16)
            late_copy(turn, line).start()

    pl.loop(0, 1)(exchange)
    if relayed:
        pl.loop(0, 1)(late)
    pl.loop(1, chunks)(exchange)
    if relayed:
        pl.loop(1, outer - 1)(late)

    first_column = lax.broadcasted_iota(jnp.int32, norm_mine.shape, 1) == 0
    for e in range(examples):
        chosen = jnp.logical_and(tile_row == e, first_column)
        ratio_ref[e] = jnp.sum(jnp.where(chosen, ratio, 0.0))

    def forward(k):
        line, sub = target(k)
        total_ref[...] = partial(line, across, sub)

        @pl.when(jnp.logical_not(is_late(line, sub)))
        def _():
            pair_copy(k).wait_recv()
            total_ref[...] += pair_in[k].astype(F32)

        if relayed:

            @pl.when(adds(line))
            def _():
                slot = (2 + lax.rem(line, 2)) * subs + sub
                landing(k, slot, line).wait_recv()
                total_ref[...] += line_in[slot].astype(F32)

        line_out[k] = total_ref[...].astype(jnp.bfloat16)
        line_copy(k).start()

    pl.loop(0, subs)(forward)

    if relayed:

        @pl.when(late_line(along))
        def _():
            own = partial(along, inner - 1 - across, subs - 1)
            for slot in range(2):
                late_landing(slot, slot, along).wait_recv()
                own = own + late_in[slot].astype(F32)
            pair_out[chunks - 1] = own.astype(jnp.bfloat16)
            pair_copy(chunks - 1).start()

    pl.loop(subs, remote)(forward)

    @pl.loop(0, subs)
    def _(sub):
        own = partial(along, across, sub)
        pair_copy(remote + sub).wait_recv()
        own = own + pair_in[remote + sub].astype(F32)
        for step in range(2 if relayed else outer - 1):
            slot = step * subs + sub
            landing(slot, slot, along).wait_recv()
            own = own + line_in[slot].astype(F32)
        into = pl.ds(pl.multiple_of(sub * rows, rows), rows)
        out_ref[into] = (own / examples_all).astype(jnp.bfloat16)

    @pl.loop(0, chunks)
    def _(k):
        line, sub = target(k)

        @pl.when(jnp.logical_not(jnp.logical_and(is_late(line, sub), k < remote)))
        def _():
            pair_copy(k).wait_send()

    if relayed:

        @pl.loop(0, outer - 1)
        def _(turn):
            line, _ = target(turn * subs)

            @pl.when(late_line(line))
            def _():
                late_copy(turn, line).wait_send()

    @pl.loop(0, remote)
    def _(k):
        line_copy(k).wait_send()


def on_device(sections, places, activations, out_grads, lengths):
    layers, examples, seq, width = activations.shape
    features = out_grads.shape[3]
    inner = 2
    outer = places // inner
    block = width // places
    rows = min(block, 128)
    subs = block // rows
    bound = 0.5 * math.sqrt(float(layers * sections * seq * width * features))
    plan = (examples, seq, outer, inner, sections, rows, subs, bound, float(places * examples))
    chunks = outer * subs
    remote = (outer - 1) * subs
    tokens = examples * seq
    tile = (max(8, -(-examples // 8) * 8), 128)
    dma = pltpu.SemaphoreType.DMA
    bf16 = jnp.bfloat16
    grad, ratio = pl.pallas_call(
        functools.partial(kernel, plan),
        out_shape=(
            jax.ShapeDtypeStruct((block, features), bf16),
            jax.ShapeDtypeStruct((examples,), F32),
        ),
        in_specs=[
            pl.BlockSpec(memory_space=pltpu.SMEM),
            pl.BlockSpec(memory_space=pl.ANY),
            pl.BlockSpec(memory_space=pl.ANY),
        ],
        out_specs=(
            pl.BlockSpec(memory_space=pltpu.VMEM),
            pl.BlockSpec(memory_space=pltpu.SMEM),
        ),
        scratch_shapes=[
            pltpu.VMEM((tokens, width), bf16),
            pltpu.VMEM((tokens, features), bf16),
            pltpu.VMEM(tile, F32),
            pltpu.VMEM((sections,) + tile, F32),
            pltpu.VMEM((chunks, rows, features), bf16),
            pltpu.VMEM((chunks, rows, features), bf16),
            pltpu.VMEM((remote, rows, features), bf16),
            pltpu.VMEM((chunks, rows, features), bf16),
            pltpu.VMEM((outer - 1, rows, features), bf16),
            pltpu.VMEM((4, rows, features), bf16),
            pltpu.VMEM((rows, features), F32),
            dma((2 * examples,)),
            dma((sections,)),
            dma((sections,)),
            dma((chunks,)),
            dma((chunks,)),
            dma((remote,)),
            dma((chunks,)),
            dma((outer - 1,)),
            dma((4,)),
        ],
        compiler_params=pltpu.CompilerParams(
            collective_id=0, has_side_effects=True, vmem_limit_bytes=56 * 2**20
        ),
    )(
        lengths,
        activations.reshape(tokens, width),
        out_grads.reshape(tokens, features),
    )
    return grad[None], ratio


def solution(mesh):
    placed = (P("section", "dp", None, None), P("section", "dp", None, None), P("dp"))
    return jax.shard_map(
        functools.partial(on_device, mesh.shape["section"], mesh.shape["dp"]),
        mesh=mesh,
        in_specs=placed,
        out_specs=(P("section", "dp", None), P("dp")),
        check_vma=False,
    )
```
